32 devices in a mesh: seq: 8 (over z, y), tensor: 4 (over x, core).
Axes of the slice: x: 2, y: 2, z: 4, core: 2. Of those that a mesh axis runs over, the one named last changes fastest.
Arguments:
- hidden_in: bfloat16 [1024, 8192], P('seq', 'tensor'), may hold values from -6 to 6
- grad_out: bfloat16 [1024, 8192], P('seq', 'tensor'), may hold values from -6 to 6
- slot_tokens: int32 [128], P('seq'), may hold values from 0 to 127, as said below
- live_counts: int32 [8], P('seq'), may hold values from 5 to 16, as said below
- norm_gain: float32 [8192], P('tensor'), may hold values from 0.5 to 1.5
- router_weight: float32 [8192], P('tensor'), may hold values from -0.0625 to 0.0625
- gate_weight: bfloat16 [8192, 24576], P('tensor', 'seq'), may hold values from -0.0625 to 0.0625
- up_weight: bfloat16 [8192, 24576], P('tensor', 'seq'), may hold values from -0.0625 to 0.0625
- down_weight: bfloat16 [24576, 8192], P('seq', 'tensor'), may hold values from -0.0390625 to 0.0390625
Outputs:
- grad_in: bfloat16 [1024, 8192], P('seq', 'tensor')
- grad_gate: bfloat16 [8192, 24576], P('tensor', 'seq')
- grad_up: bfloat16 [8192, 24576], P('tensor', 'seq')
- grad_down: bfloat16 [24576, 8192], P('seq', 'tensor')
- grad_gain: float32 [8192], P('tensor')
- grad_router: float32 [8192], P('tensor')
The draws below stay inside these ranges and needn't reach their ends.
Inputs may be any that keep to these rules, and one draw needn't show every extreme that they name: `slot_tokens`: slot p belongs to index p // 16 of seq; the live slots of one index hold distinct positions, the others hold arbitrary positions of that index. `live_counts`: in every draw some index of seq has all 16 slots live.
All inputs are finite; a program needn't handle non-finite values.
Results may differ from the reference program's by a relative error of at most 0.0077.
Values may be sent and summed in bfloat16 or wider, within the bound.
A program may use at most 128 MiB of HBM per device.

```python
import jax
import jax.numpy as jnp
from jax import lax

D = 8192
FF = 24576
TOK_DEV = 128
CAP = 16
TOKENS = 1024
N_SEQ = 8


def routing_draw(key):
    base = jax.random.fold_in(key, 11)
    first, second, third, fourth = jax.random.split(base, 4)
    lowest = max(CAP // 3, 1)
    ranks = jnp.arange(N_SEQ, dtype=jnp.int32)
    floors = lowest + (CAP - lowest) * ranks // max(N_SEQ - 1, 1)
    counts = jax.random.randint(first, (N_SEQ,), floors, CAP + 1, dtype=jnp.int32)
    chosen = jax.random.randint(second, (), 0, N_SEQ, dtype=jnp.int32)
    counts = jnp.where(ranks == chosen, CAP, counts).astype(jnp.int32)
    keys = jax.random.split(third, N_SEQ)
    orders = jax.vmap(lambda single: jax.random.permutation(single, TOK_DEV))(keys)[:, :CAP].astype(jnp.int32)
    filler = jax.random.randint(fourth, (N_SEQ, CAP), 0, TOK_DEV, dtype=jnp.int32)
    columns = jnp.arange(CAP, dtype=jnp.int32)[None, :]
    tokens = jnp.where(columns < counts[:, None], orders, filler).reshape(-1).astype(jnp.int32)
    return (tokens, counts)


def draw_slot_tokens(key, part):
    return routing_draw(key)[0]


def draw_live_counts(key, part):
    return routing_draw(key)[1]


def block_scale(own_key, shape, pieces, least, top_value):
    def one(dim, blocks):
        heights = jax.random.uniform(jax.random.fold_in(jax.random.fold_in(own_key, 6), dim), (blocks,), jnp.float32, least / len(pieces), top_value / len(pieces))
        return jnp.repeat(jnp.exp(heights), shape[dim] // blocks).reshape((-1,) + (1,) * (len(shape) - dim - 1))

    loudness = one(*pieces[0])
    for cut in pieces[1:]:
        loudness = loudness * one(*cut)
    return loudness


def centred(stream_key, extent, spread, bound, cuts=(), kind=jnp.bfloat16):
    array = jax.random.normal(stream_key, extent, jnp.float32) * spread
    if len(cuts) > 0:
        array = block_scale(stream_key, extent, cuts, -0.22, 0.18) * array
    return jnp.clip(array, min=-bound, max=bound).astype(kind)


def setup_inputs(seed: int = 0) -> dict:
    key_list = jax.random.split(jax.random.key(seed), 10)
    return {
        "hidden_in": centred(key_list[0], (TOKENS, D), 1.0, 6.0, ((0, 8), (1, 4))),
        "grad_out": centred(key_list[1], (TOKENS, D), 1.0, 6.0, ((0, 8), (1, 4))),
        "slot_tokens": draw_slot_tokens(jax.random.fold_in(key_list[9], 71), 0),
        "live_counts": draw_live_counts(jax.random.fold_in(key_list[9], 71), 0),
        "norm_gain": jnp.clip(1.0 + 0.1 * jax.random.normal(key_list[4], (D,), jnp.float32), 0.5, 1.5),
        "router_weight": centred(key_list[5], (D,), D ** -0.5, 0.0625, ((0, 4),), jnp.float32),
        "gate_weight": centred(key_list[6], (D, FF), D ** -0.5, 0.0625, ((0, 4), (1, 8))),
        "up_weight": centred(key_list[7], (D, FF), D ** -0.5, 0.0625, ((0, 4), (1, 8))),
        "down_weight": centred(key_list[8], (FF, D), FF ** -0.5, 0.0390625, ((0, 8), (1, 4))),
    }


norm_eps = 1e-06

def silu_parts(gate):
    sig = jax.nn.sigmoid(gate)
    return (gate * sig, sig * (1.0 + gate * (1.0 - sig)))

def reference(hidden_in, grad_out, slot_tokens, live_counts, norm_gain, router_weight, gate_weight, up_weight, down_weight):
    slots = jnp.arange(N_SEQ * CAP, dtype=jnp.int32)
    owners = slots // CAP
    positions = (owners * TOK_DEV + slot_tokens).astype(jnp.int32)
    live_rows = slots % CAP < live_counts[owners]
    picked = jnp.take(hidden_in, positions, axis=0)
    upstream = jnp.where(live_rows[:, None], jnp.take(grad_out, positions, axis=0), jnp.zeros((), jnp.bfloat16))
    wide = picked.astype(jnp.float32)
    inverse = lax.rsqrt(lax.optimization_barrier(jnp.mean(wide * wide, axis=1, keepdims=True)) + norm_eps)
    scaled = wide * inverse
    normed = (scaled * norm_gain).astype(jnp.bfloat16)
    logits = jnp.dot(normed, router_weight.astype(jnp.bfloat16), preferred_element_type=jnp.float32)
    gate = jnp.dot(normed, gate_weight, preferred_element_type=jnp.float32)
    upper = jnp.dot(normed, up_weight, preferred_element_type=jnp.float32)
    back = jnp.dot(upstream, down_weight.T, preferred_element_type=jnp.float32)
    act, slope = silu_parts(gate)
    hidden = act * upper
    weighted = (hidden * logits[:, None]).astype(jnp.bfloat16)
    router_grad = lax.optimization_barrier(jnp.sum(hidden * back, axis=1))
    d_hidden = logits[:, None] * back
    d_gate = (d_hidden * upper * slope).astype(jnp.bfloat16)
    d_up = (d_hidden * act).astype(jnp.bfloat16)
    count_scale = lax.rsqrt(jnp.sum(live_counts).astype(jnp.float32))
    grad_gate = (count_scale * jnp.dot(normed.T, d_gate, preferred_element_type=jnp.float32)).astype(jnp.bfloat16)
    grad_up = (count_scale * jnp.dot(normed.T, d_up, preferred_element_type=jnp.float32)).astype(jnp.bfloat16)
    grad_down = (count_scale * jnp.dot(weighted.T, upstream, preferred_element_type=jnp.float32)).astype(jnp.bfloat16)
    d_normed = jnp.dot(d_gate, gate_weight.T, preferred_element_type=jnp.float32)
    d_normed = d_normed + jnp.dot(d_up, up_weight.T, preferred_element_type=jnp.float32)
    d_normed = d_normed + router_grad[:, None] * router_weight
    grad_gain = count_scale * lax.optimization_barrier(jnp.sum(d_normed * scaled, axis=0))
    grad_router = count_scale * jnp.dot(router_grad, normed.astype(jnp.float32), precision=lax.Precision.HIGHEST)
    d_scaled = d_normed * norm_gain
    d_picked = inverse * (d_scaled - scaled * lax.optimization_barrier(jnp.mean(d_scaled * scaled, axis=1, keepdims=True)))
    d_picked = jnp.where(live_rows[:, None], d_picked, jnp.zeros((), jnp.float32))
    grad_in = grad_out.astype(jnp.float32).at[positions].add(d_picked).astype(jnp.bfloat16)
    return (grad_in, grad_gate, grad_up, grad_down, grad_gain, grad_router)
```

```python
import functools

import jax
import jax.numpy as jnp
from jax import lax
from jax.experimental import pallas as pl
from jax.experimental.pallas import tpu as pltpu
from jax.sharding import PartitionSpec as P

norm_eps = 1e-06
f32 = jnp.float32
bf16 = jnp.bfloat16
MESH = pl.DeviceIdType.MESH


def pick_chunks(size, options, unit=128):
    for n in options:
        if size % (n * unit) == 0:
            return n
    return 1


def nt_dot(a, b):
    return lax.dot_general(a, b, (((1,), (1,)), ((), ())), preferred_element_type=f32)


def kernel(
    ns,
    nt,
    nc,
    nk,
    hid,
    gout,
    tok_col,
    tok_row,
    live,
    gain,
    router,
    wg_hbm,
    wu_hbm,
    wd_hbm,
    o_in,
    o_gr,
    o_w,
    o_dg,
    o_du,
    o_norm,
    o_ups,
    o_cs,
    wg,
    wu,
    wd,
    gath,
    colbuf,
    invbuf,
    logbuf,
    rgbuf,
    rgacc,
    smsg,
    srec,
    imsg,
    irec,
    part,
    drec,
    xsnd,
    xrec,
    acc,
    ysnd,
    yrec,
    zsnd,
    zrec,
    gmsg,
    grec,
    w_sem,
    agz_s,
    agz_r,
    agy_s,
    agy_r,
    sm_s,
    sm_r,
    in_s,
    in_r,
    d_s,
    d_r,
    x_s,
    x_r,
    a_s,
    a_r,
    rg_s,
    rg_r,
    y_s,
    y_r,
    z_s,
    z_r,
    g_s,
    g_r,
):
    tokens, width = hid.shape
    cap = tok_col.shape[0]
    rows = ns * cap
    half = rows // 2
    hidden = wg.shape[1]
    fc = hidden // nc
    kc = width // nk
    nz, nx = ns // 2, nt // 2
    s, t = lax.axis_index("seq"), lax.axis_index("tensor")
    y, z = lax.rem(s, 2), lax.div(s, 2)
    core, x = lax.rem(t, 2), lax.div(t, 2)
    mate = t + 1 - 2 * core
    yp = s + 1 - 2 * y
    mine = pl.multiple_of(core * half, half)

    def remote(src, dst, ssem, rsem, **where):
        return pltpu.make_async_remote_copy(
            src_ref=src,
            dst_ref=dst,
            send_sem=ssem,
            recv_sem=rsem,
            device_id=where,
            device_id_type=MESH,
        )

    loads = [
        pltpu.make_async_copy(wd_hbm, wd, w_sem.at[0]),
        pltpu.make_async_copy(wg_hbm, wg, w_sem.at[1]),
        pltpu.make_async_copy(wu_hbm, wu, w_sem.at[2]),
    ]
    for load in loads:
        load.start()

    barrier = pltpu.get_barrier_semaphore()
    for j in range(1, ns):
        pl.semaphore_signal(
            barrier, inc=1, device_id={"seq": lax.rem(s + j, ns)}, device_id_type=MESH
        )
    for j in range(1, nt):
        pl.semaphore_signal(
            barrier, inc=1, device_id={"tensor": lax.rem(t + j, nt)}, device_id_type=MESH
        )

    hot = (tok_col[...] == lax.broadcasted_iota(jnp.int32, (cap, tokens), 1)).astype(f32)
    live_col = (lax.broadcasted_iota(jnp.int32, (cap, 1), 0) < live[...]).astype(f32)
    gath[s, :, pl.ds(0, width)] = jnp.dot(
        hot.astype(bf16), hid[...], preferred_element_type=f32
    ).astype(bf16)
    gath[s, :, pl.ds(width, width)] = jnp.dot(
        (hot * live_col).astype(bf16), gout[...], preferred_element_type=f32
    ).astype(bf16)
    gath[s, :, pl.ds(2 * width, 128)] = jnp.broadcast_to(
        live[...].astype(f32), (cap, 128)
    ).astype(bf16)
    pl.semaphore_wait(barrier, ns - 1 + nt - 1)

    def agz(j):
        own = gath.at[s]
        return remote(own, own, agz_s.at[j], agz_r.at[j], seq=2 * lax.rem(z + j, nz) + y)

    def agy(j):
        block = gath.at[2 * lax.rem(z + nz - j, nz) + y]
        return remote(block, block, agy_s.at[j], agy_r.at[j], seq=yp)

    def consume(b):
        rows_b = pl.ds(pl.multiple_of(b * cap, cap), cap)
        wide = gath[b, :, pl.ds(0, width)].astype(f32)
        o_ups[rows_b, :] = gath[b, :, pl.ds(width, width)]
        colbuf[rows_b, :] = jnp.broadcast_to(
            jnp.sum(wide * wide, axis=1, keepdims=True), (cap, 128)
        )

    agy(0).start()
    for j in range(1, nz):
        agz(j).start()
    consume(s)

    @pl.loop(1, nz)
    def _(j):
        agz(j).wait_recv()
        agy(j).start()
        consume(2 * lax.rem(z + nz - j, nz) + y)

    @pl.loop(0, nz)
    def _(j):
        agy(j).wait_recv()
        consume(2 * lax.rem(z + nz - j, nz) + 1 - y)

    def small(k, j):
        return remote(
            smsg.at[k], srec.at[k, j], sm_s.at[k, j], sm_r.at[k, j], tensor=lax.rem(t + j, nt)
        )

    def small_send(k):
        smsg[k] = colbuf[...].T[0:8, :]
        for j in range(1, nt):
            small(k, j).start()

    def small_sum(k):
        total = smsg[k]
        for j in range(1, nt):
            small(k, j).wait_recv()
            total = total + srec[k, j]
        return jnp.broadcast_to(total[0:1, :], (128, rows)).T

    small_send(0)

    def pair(a, c):
        return remote(
            part.at[a, c, 1 - core], drec.at[a, c], d_s.at[a, c], d_r.at[a, c], tensor=mate
        )

    def cross(j, a, c):
        return remote(
            xsnd.at[a, c],
            xrec.at[j, a, c],
            x_s.at[j, a, c],
            x_r.at[j, a, c],
            tensor=2 * lax.rem(x + j, nx) + core,
        )

    def emit(a, c, value):
        part[a, c] = value.reshape(2, half, fc)
        pair(a, c).start()

    def relay(a, c):
        pair(a, c).wait_recv()
        total = part[a, c, core] + drec[a, c]
        part[a, c, core] = total
        xsnd[a, c] = total.astype(bf16)
        for j in range(1, nx):
            cross(j, a, c).start()

    def cols(c):
        return pl.ds(pl.multiple_of(c * fc, fc), fc)

    loads[0].wait()

    @pl.loop(0, nc)
    def _(c):
        emit(0, c, nt_dot(o_ups[...], wd[cols(c), :]))

        @pl.when(c > 0)
        def _():
            relay(0, c - 1)

    relay(0, nc - 1)

    width_total = width * nt
    invbuf[...] = lax.rsqrt(small_sum(0) / width_total + norm_eps)
    router_row = router[...].astype(bf16).astype(f32)

    @pl.loop(0, ns)
    def _(b):
        rows_b = pl.ds(pl.multiple_of(b * cap, cap), cap)
        scaled = gath[b, :, pl.ds(0, width)].astype(f32) * invbuf[rows_b, 0:1]
        normed = (scaled * gain[...]).astype(bf16)
        o_norm[rows_b, :] = normed
        colbuf[rows_b, :] = jnp.broadcast_to(
            jnp.sum(normed.astype(f32) * router_row, axis=1, keepdims=True), (cap, 128)
        )

    small_send(1)
    loads[1].wait()
    loads[2].wait()

    @pl.loop(0, nc)
    def _(c):
        emit(1, c, jnp.dot(o_norm[...], wg[:, cols(c)], preferred_element_type=f32))

        @pl.when(c > 0)
        def _():
            relay(2, c - 1)

        emit(2, c, jnp.dot(o_norm[...], wu[:, cols(c)], preferred_element_type=f32))
        relay(1, c)

    relay(2, nc - 1)

    logbuf[...] = small_sum(1)
    rgacc[...] = jnp.zeros_like(rgacc)
    acc[...] = jnp.zeros_like(acc)
    acts = (o_w, o_dg, o_du)

    def act_copy(a, c):
        piece = acts[a].at[pl.ds(mine, half), cols(c)]
        return remote(piece, piece, a_s.at[a, c], a_r.at[a, c], tensor=mate)

    def gate_backward(c):
        for a in range(3):
            for j in range(1, nx):
                cross(j, a, c).wait_recv()

        @pl.loop(0, half // 16)
        def _(r):
            sub = pl.ds(pl.multiple_of(r * 16, 16), 16)
            out = pl.ds(pl.multiple_of(mine + r * 16, 16), 16)
            back, gate, upper = [
                functools.reduce(
                    lambda u, v: u + v,
                    [xrec[j, a, c, sub, :].astype(f32) for j in range(1, nx)],
                    part[a, c, core, sub, :],
                )
                for a in range(3)
            ]
            logit = logbuf[out, 0:1]
            sig = jax.nn.sigmoid(gate)
            act = gate * sig
            slope = sig * (1.0 + gate * (1.0 - sig))
            hid_v = act * upper
            o_w[out, cols(c)] = (hid_v * logit).astype(bf16)
            d_hidden = logit * back
            o_dg[out, cols(c)] = (d_hidden * upper * slope).astype(bf16)
            o_du[out, cols(c)] = (d_hidden * act).astype(bf16)
            terms = hid_v * back
            add = terms[:, 0:128]
            for i in range(1, fc // 128):
                add = add + terms[:, i * 128 : (i + 1) * 128]
            rgacc[sub, :] = rgacc[sub, :] + add

        for a in range(3):
            act_copy(a, c).start()

    def kcols(k):
        return pl.ds(pl.multiple_of(k * kc, kc), kc)

    def back_dots(c, k):
        return nt_dot(o_dg[:, cols(c)], wg[kcols(k), cols(c)]) + nt_dot(
            o_du[:, cols(c)], wu[kcols(k), cols(c)]
        )

    def act_wait(c):
        for a in range(3):
            act_copy(a, c).wait_recv()

    @pl.loop(0, nc)
    def _(c):
        gate_backward(c)

        @pl.when(c > 0)
        def _():
            act_wait(c - 1)

            @pl.loop(0, nk)
            def _(k):
                acc[:, :, kcols(k)] = acc[:, :, kcols(k)] + back_dots(c - 1, k).reshape(
                    ns, cap, kc
                )

    rgbuf[core] = jnp.broadcast_to(jnp.sum(rgacc[...], axis=1, keepdims=True), (half, 128))
    rg_copy = remote(rgbuf.at[core], rgbuf.at[core], rg_s, rg_r, tensor=mate)
    rg_copy.start()
    act_wait(nc - 1)
    rg_copy.wait_recv()

    def ycopy(k):
        return remote(ysnd.at[k], yrec.at[k], y_s.at[k], y_r.at[k], seq=yp)

    def zcopy(j, k):
        return remote(
            zsnd.at[j, k],
            zrec.at[j, k],
            z_s.at[j, k],
            z_r.at[j, k],
            seq=2 * lax.rem(z + j, nz) + y,
        )

    def zstage(k):
        ycopy(k).wait_recv()
        for j in range(1, nz):
            zz = lax.rem(z + j, nz)
            zsnd[j, k] = (acc[2 * zz + y, :, kcols(k)] + yrec[k, zz].astype(f32)).astype(bf16)
            zcopy(j, k).start()
        acc[s, :, kcols(k)] = acc[s, :, kcols(k)] + yrec[k, z].astype(f32)

    @pl.loop(0, nk)
    def _(k):
        rg = jnp.concatenate([rgbuf[0], rgbuf[1]], axis=0)[:, 0:1]
        total = back_dots(nc - 1, k) + rg * router[:, kcols(k)]
        acc[:, :, kcols(k)] = acc[:, :, kcols(k)] + total.reshape(ns, cap, kc)
        for zz in range(nz):
            ysnd[k, zz] = acc[2 * zz + 1 - y, :, kcols(k)].astype(bf16)
        ycopy(k).start()

        @pl.when(k > 0)
        def _():
            zstage(k - 1)

    zstage(nk - 1)

    router_part = jnp.zeros((1, width), f32)
    count = jnp.zeros((1, 128), f32)
    rg_all = jnp.concatenate([rgbuf[0], rgbuf[1]], axis=0)
    for b in range(ns):
        block = o_norm[b * cap : (b + 1) * cap, :].astype(f32)
        router_part = router_part + jnp.sum(
            rg_all[b * cap : (b + 1) * cap, 0:1] * block, axis=0, keepdims=True
        )
        count = count + gath[b, 0:1, 2 * width : 2 * width + 128].astype(f32)
    scale = lax.rsqrt(count)
    o_cs[...] = scale
    gmsg[1:2, :] = router_part

    for j in range(1, nz):

        @pl.loop(0, nk)
        def _(k):
            zcopy(j, k).wait_recv()
            acc[s, :, kcols(k)] = acc[s, :, kcols(k)] + zrec[j, k].astype(f32)

    own = pl.ds(pl.multiple_of(s * cap, cap), cap)
    inverse = invbuf[own, 0:1]
    scaled = gath[s, :, pl.ds(0, width)].astype(f32) * inverse
    d_normed = acc[s]
    d_scaled = d_normed * gain[...]
    imsg[...] = jnp.broadcast_to(jnp.sum(d_scaled * scaled, axis=1, keepdims=True), (cap, 128))

    def inner_copy(j):
        return remote(imsg, irec.at[j], in_s.at[j], in_r.at[j], tensor=lax.rem(t + j, nt))

    def gain_copy(j):
        return remote(gmsg, grec.at[j], g_s.at[j], g_r.at[j], seq=lax.rem(s + j, ns))

    for j in range(1, nt):
        inner_copy(j).start()
    gmsg[0:1, :] = jnp.sum(d_normed * scaled, axis=0, keepdims=True)
    for j in range(1, ns):
        gain_copy(j).start()

    inner = imsg[...]
    for j in range(1, nt):
        inner_copy(j).wait_recv()
        inner = inner + irec[j]
    inner = inner[:, 0:1] / width_total
    d_picked = inverse * (d_scaled - scaled * inner) * live_col
    place = (tok_row[...] == lax.broadcasted_iota(jnp.int32, (tokens, cap), 0)).astype(f32)
    added = jnp.dot(place, d_picked, precision=lax.Precision.HIGHEST, preferred_element_type=f32)
    o_in[...] = (gout[...].astype(f32) + added).astype(bf16)

    total = gmsg[...]
    for j in range(1, ns):
        gain_copy(j).wait_recv()
        total = total + grec[j]
    o_gr[...] = total * scale[:, 0:1]

    agy(0).wait_send()
    for j in range(1, nz):
        agz(j).wait_send()
        agy(j).wait_send()
    for j in range(1, nt):
        small(0, j).wait_send()
        small(1, j).wait_send()
        inner_copy(j).wait_send()
    for j in range(1, ns):
        gain_copy(j).wait_send()
    rg_copy.wait_send()

    @pl.loop(0, nc)
    def _(c):
        for a in range(3):
            pair(a, c).wait_send()
            act_copy(a, c).wait_send()
            for j in range(1, nx):
                cross(j, a, c).wait_send()

    @pl.loop(0, nk)
    def _(k):
        ycopy(k).wait_send()
        for j in range(1, nz):
            zcopy(j, k).wait_send()


def body(
    hidden_in,
    grad_out,
    slot_tokens,
    live_counts,
    norm_gain,
    router_weight,
    gate_weight,
    up_weight,
    down_weight,
):
    ns, nt = lax.axis_size("seq"), lax.axis_size("tensor")
    cap = slot_tokens.shape[0]
    tokens, width = hidden_in.shape
    hidden = gate_weight.shape[1]
    rows, nz, nx = ns * cap, ns // 2, nt // 2
    half = rows // 2
    nc = pick_chunks(hidden, (6, 4, 3, 2))
    nk = pick_chunks(width, (4, 2))
    fc, kc = hidden // nc, width // nk
    vmem = pl.BlockSpec(memory_space=pltpu.VMEM)
    hbm = pl.BlockSpec(memory_space=pl.ANY)
    dma = pltpu.SemaphoreType.DMA
    grad_in, small, weighted, d_gate, d_up, normed, upstream, scale = pl.pallas_call(
        functools.partial(kernel, ns, nt, nc, nk),
        out_shape=[
            jax.ShapeDtypeStruct((tokens, width), bf16),
            jax.ShapeDtypeStruct((2, width), f32),
            jax.ShapeDtypeStruct((rows, hidden), bf16),
            jax.ShapeDtypeStruct((rows, hidden), bf16),
            jax.ShapeDtypeStruct((rows, hidden), bf16),
            jax.ShapeDtypeStruct((rows, width), bf16),
            jax.ShapeDtypeStruct((rows, width), bf16),
            jax.ShapeDtypeStruct((1, 128), f32),
        ],
        in_specs=[vmem] * 7 + [hbm] * 3,
        out_specs=[vmem] * 8,
        scratch_shapes=[
            pltpu.VMEM((width, hidden), bf16),
            pltpu.VMEM((width, hidden), bf16),
            pltpu.VMEM((hidden, width), bf16),
            pltpu.VMEM((ns, cap, 2 * width + 128), bf16),
            pltpu.VMEM((rows, 128), f32),
            pltpu.VMEM((rows, 128), f32),
            pltpu.VMEM((rows, 128), f32),
            pltpu.VMEM((2, half, 128), f32),
            pltpu.VMEM((half, 128), f32),
            pltpu.VMEM((2, 8, rows), f32),
            pltpu.VMEM((2, nt, 8, rows), f32),
            pltpu.VMEM((cap, 128), f32),
            pltpu.VMEM((nt, cap, 128), f32),
            pltpu.VMEM((3, nc, 2, half, fc), f32),
            pltpu.VMEM((3, nc, half, fc), f32),
            pltpu.VMEM((3, nc, half, fc), bf16),
            pltpu.VMEM((nx, 3, nc, half, fc), bf16),
            pltpu.VMEM((ns, cap, width), f32),
            pltpu.VMEM((nk, nz, cap, kc), bf16),
            pltpu.VMEM((nk, nz, cap, kc), bf16),
            pltpu.VMEM((nz, nk, cap, kc), bf16),
            pltpu.VMEM((nz, nk, cap, kc), bf16),
            pltpu.VMEM((2, width), f32),
            pltpu.VMEM((ns, 2, width), f32),
            dma((3,)),
            dma((nz,)),
            dma((nz,)),
            dma((nz,)),
            dma((nz,)),
            dma((2, nt)),
            dma((2, nt)),
            dma((nt,)),
            dma((nt,)),
            dma((3, nc)),
            dma((3, nc)),
            dma((nx, 3, nc)),
            dma((nx, 3, nc)),
            dma((3, nc)),
            dma((3, nc)),
            dma,
            dma,
            dma((nk,)),
            dma((nk,)),
            dma((nz, nk)),
            dma((nz, nk)),
            dma((ns,)),
            dma((ns,)),
        ],
        compiler_params=pltpu.CompilerParams(
            collective_id=0, has_side_effects=True, vmem_limit_bytes=67_043_328
        ),
    )(
        hidden_in,
        grad_out,
        slot_tokens.reshape(cap, 1),
        slot_tokens.reshape(1, cap),
        live_counts.reshape(1, 1),
        norm_gain.reshape(1, width),
        router_weight.reshape(1, width),
        gate_weight,
        up_weight,
        down_weight,
    )
    count_scale = scale[0, 0]
    grad_gate = jnp.einsum("pd,pf->df", normed, d_gate, preferred_element_type=f32)
    grad_up = jnp.einsum("pd,pf->df", normed, d_up, preferred_element_type=f32)
    grad_down = jnp.einsum("pf,pd->fd", weighted, upstream, preferred_element_type=f32)
    return (
        grad_in,
        (count_scale * grad_gate).astype(bf16),
        (count_scale * grad_up).astype(bf16),
        (count_scale * grad_down).astype(bf16),
        small[0],
        small[1],
    )


def solution(mesh):
    in_specs = (
        P("seq", "tensor"),
        P("seq", "tensor"),
        P("seq"),
        P("seq"),
        P("tensor"),
        P("tensor"),
        P("tensor", "seq"),
        P("tensor", "seq"),
        P("seq", "tensor"),
    )
    out_specs = (
        P("seq", "tensor"),
        P("tensor", "seq"),
        P("tensor", "seq"),
        P("seq", "tensor"),
        P("tensor"),
        P("tensor"),
    )
    return jax.shard_map(body, mesh=mesh, in_specs=in_specs, out_specs=out_specs, check_vma=False)
```

```python
import functools

import jax
import jax.numpy as jnp
from jax import lax
from jax.experimental import pallas as pl
from jax.experimental.pallas import tpu as pltpu
from jax.sharding import PartitionSpec as P

norm_eps = 1e-06
f32 = jnp.float32
bf16 = jnp.bfloat16
MESH = pl.DeviceIdType.MESH


def pick_chunks(size, options, unit=128):
    for n in options:
        if size % (n * unit) == 0:
            return n
    return 1


def nt_dot(a, b):
    return lax.dot_general(a, b, (((1,), (1,)), ((), ())), preferred_element_type=f32)


def tn_dot(a, b):
    return lax.dot_general(a, b, (((0,), (0,)), ((), ())), preferred_element_type=f32)


def outer_kernel(norm, dg, du, wt, ups, cs, o_gate, o_up, o_down):
    scale = cs[0:1, 0:1]

    def fill(out, left, right):
        size = right.shape[1]
        piece = size // pick_chunks(size, (6, 4, 3, 2))
        for n in range(0, size, piece):
            out[:, n : n + piece] = (tn_dot(left, right[:, n : n + piece]) * scale).astype(bf16)

    fill(o_gate, norm[...], dg)
    fill(o_up, norm[...], du)
    fill(o_down, wt[...], ups)


def outer_products(normed, d_gate, d_up, weighted, upstream, scale):
    rows, width = normed.shape
    hidden = d_gate.shape[1]
    steps = next(n for n in (8, 4, 2, 1) if width % (n * 128) == 0 and hidden % (n * 128) == 0)
    tw, th = width // steps, hidden // steps

    def whole(shape):
        return pl.BlockSpec(shape, lambda i: (0, 0))

    return pl.pallas_call(
        outer_kernel,
        grid=(steps,),
        out_shape=[
            jax.ShapeDtypeStruct((width, hidden), bf16),
            jax.ShapeDtypeStruct((width, hidden), bf16),
            jax.ShapeDtypeStruct((hidden, width), bf16),
        ],
        in_specs=[
            pl.BlockSpec((rows, tw), lambda i: (0, i)),
            whole((rows, hidden)),
            whole((rows, hidden)),
            pl.BlockSpec((rows, th), lambda i: (0, i)),
            whole((rows, width)),
            whole((1, 128)),
        ],
        out_specs=[
            pl.BlockSpec((tw, hidden), lambda i: (i, 0)),
            pl.BlockSpec((tw, hidden), lambda i: (i, 0)),
            pl.BlockSpec((th, width), lambda i: (i, 0)),
        ],
        compiler_params=pltpu.CompilerParams(
            dimension_semantics=("arbitrary",), vmem_limit_bytes=67_043_328
        ),
    )(normed, d_gate, d_up, weighted, upstream, scale)


def kernel(
    ns,
    nt,
    nc,
    nk,
    hid,
    gout,
    tok_col,
    tok_row,
    live,
    gain,
    router,
    wg_hbm,
    wu_hbm,
    wd_hbm,
    o_in,
    o_gr,
    o_w,
    o_dg,
    o_du,
    o_norm,
    o_ups,
    o_cs,
    wg,
    wu,
    wd,
    gath,
    colbuf,
    invbuf,
    logbuf,
    rgbuf,
    rgacc,
    smsg,
    srec,
    imsg,
    irec,
    part,
    drec,
    xsnd,
    xrec,
    acc,
    ysnd,
    yrec,
    zsnd,
    zrec,
    gmsg,
    grec,
    w_sem,
    agz_s,
    agz_r,
    agy_s,
    agy_r,
    sm_s,
    sm_r,
    in_s,
    in_r,
    d_s,
    d_r,
    x_s,
    x_r,
    a_s,
    a_r,
    rg_s,
    rg_r,
    y_s,
    y_r,
    z_s,
    z_r,
    g_s,
    g_r,
):
    tokens, width = hid.shape
    cap = tok_col.shape[0]
    rows = ns * cap
    half = rows // 2
    hidden = wg.shape[1]
    fc = hidden // nc
    kc = width // nk
    nz, nx = ns // 2, nt // 2
    s, t = lax.axis_index("seq"), lax.axis_index("tensor")
    y, z = lax.rem(s, 2), lax.div(s, 2)
    core, x = lax.rem(t, 2), lax.div(t, 2)
    mate = t + 1 - 2 * core
    yp = s + 1 - 2 * y
    mine = pl.multiple_of(core * half, half)

    def remote(src, dst, ssem, rsem, **where):
        return pltpu.make_async_remote_copy(
            src_ref=src,
            dst_ref=dst,
            send_sem=ssem,
            recv_sem=rsem,
            device_id=where,
            device_id_type=MESH,
        )

    loads = [
        pltpu.make_async_copy(wd_hbm, wd, w_sem.at[0]),
        pltpu.make_async_copy(wg_hbm, wg, w_sem.at[1]),
        pltpu.make_async_copy(wu_hbm, wu, w_sem.at[2]),
    ]
    for load in loads:
        load.start()

    barrier = pltpu.get_barrier_semaphore()
    for j in range(1, ns):
        pl.semaphore_signal(
            barrier, inc=1, device_id={"seq": lax.rem(s + j, ns)}, device_id_type=MESH
        )
    for j in range(1, nt):
        pl.semaphore_signal(
            barrier, inc=1, device_id={"tensor": lax.rem(t + j, nt)}, device_id_type=MESH
        )

    hot = (tok_col[...] == lax.broadcasted_iota(jnp.int32, (cap, tokens), 1)).astype(f32)
    live_col = (lax.broadcasted_iota(jnp.int32, (cap, 1), 0) < live[...]).astype(f32)
    gath[s, :, pl.ds(0, width)] = jnp.dot(
        hot.astype(bf16), hid[...], preferred_element_type=f32
    ).astype(bf16)
    gath[s, :, pl.ds(width, width)] = jnp.dot(
        (hot * live_col).astype(bf16), gout[...], preferred_element_type=f32
    ).astype(bf16)
    gath[s, :, pl.ds(2 * width, 128)] = jnp.broadcast_to(
        live[...].astype(f32), (cap, 128)
    ).astype(bf16)
    pl.semaphore_wait(barrier, ns - 1 + nt - 1)

    def agz(j):
        own = gath.at[s]
        return remote(own, own, agz_s.at[j], agz_r.at[j], seq=2 * lax.rem(z + j, nz) + y)

    def agy(j):
        block = gath.at[2 * lax.rem(z + nz - j, nz) + y]
        return remote(block, block, agy_s.at[j], agy_r.at[j], seq=yp)

    def consume(b):
        rows_b = pl.ds(pl.multiple_of(b * cap, cap), cap)
        wide = gath[b, :, pl.ds(0, width)].astype(f32)
        o_ups[rows_b, :] = gath[b, :, pl.ds(width, width)]
        colbuf[rows_b, :] = jnp.broadcast_to(
            jnp.sum(wide * wide, axis=1, keepdims=True), (cap, 128)
        )

    agy(0).start()
    for j in range(1, nz):
        agz(j).start()
    consume(s)

    @pl.loop(1, nz)
    def _(j):
        agz(j).wait_recv()
        agy(j).start()
        consume(2 * lax.rem(z + nz - j, nz) + y)

    @pl.loop(0, nz)
    def _(j):
        agy(j).wait_recv()
        consume(2 * lax.rem(z + nz - j, nz) + 1 - y)

    def small(k, j):
        return remote(
            smsg.at[k], srec.at[k, j], sm_s.at[k, j], sm_r.at[k, j], tensor=lax.rem(t + j, nt)
        )

    def small_send(k):
        smsg[k] = colbuf[...].T[0:8, :]
        for j in range(1, nt):
            small(k, j).start()

    def small_sum(k):
        total = smsg[k]
        for j in range(1, nt):
            small(k, j).wait_recv()
            total = total + srec[k, j]
        return jnp.broadcast_to(total[0:1, :], (128, rows)).T

    small_send(0)

    def pair(a, c):
        return remote(
            part.at[a, c, 1 - core], drec.at[a, c], d_s.at[a, c], d_r.at[a, c], tensor=mate
        )

    def cross(j, a, c):
        return remote(
            xsnd.at[a, c],
            xrec.at[j, a, c],
            x_s.at[j, a, c],
            x_r.at[j, a, c],
            tensor=2 * lax.rem(x + j, nx) + core,
        )

    def emit(a, c, value):
        part[a, c] = value.reshape(2, half, fc)
        pair(a, c).start()

    def relay(a, c):
        pair(a, c).wait_recv()
        total = part[a, c, core] + drec[a, c]
        part[a, c, core] = total
        xsnd[a, c] = total.astype(bf16)
        for j in range(1, nx):
            cross(j, a, c).start()

    def cols(c):
        return pl.ds(pl.multiple_of(c * fc, fc), fc)

    loads[0].wait()

    @pl.loop(0, nc)
    def _(c):
        emit(0, c, nt_dot(o_ups[...], wd[cols(c), :]))

        @pl.when(c > 0)
        def _():
            relay(0, c - 1)

    relay(0, nc - 1)

    width_total = width * nt
    invbuf[...] = lax.rsqrt(small_sum(0) / width_total + norm_eps)
    router_row = router[...].astype(bf16).astype(f32)

    @pl.loop(0, ns)
    def _(b):
        rows_b = pl.ds(pl.multiple_of(b * cap, cap), cap)
        scaled = gath[b, :, pl.ds(0, width)].astype(f32) * invbuf[rows_b, 0:1]
        normed = (scaled * gain[...]).astype(bf16)
        o_norm[rows_b, :] = normed
        colbuf[rows_b, :] = jnp.broadcast_to(
            jnp.sum(normed.astype(f32) * router_row, axis=1, keepdims=True), (cap, 128)
        )

    small_send(1)
    loads[1].wait()
    loads[2].wait()

    @pl.loop(0, nc)
    def _(c):
        emit(1, c, jnp.dot(o_norm[...], wg[:, cols(c)], preferred_element_type=f32))

        @pl.when(c > 0)
        def _():
            relay(2, c - 1)

        emit(2, c, jnp.dot(o_norm[...], wu[:, cols(c)], preferred_element_type=f32))
        relay(1, c)

    relay(2, nc - 1)

    logbuf[...] = small_sum(1)
    rgacc[...] = jnp.zeros_like(rgacc)
    acc[...] = jnp.zeros_like(acc)
    acts = (o_w, o_dg, o_du)

    def act_copy(a, c):
        piece = acts[a].at[pl.ds(mine, half), cols(c)]
        return remote(piece, piece, a_s.at[a, c], a_r.at[a, c], tensor=mate)

    def gate_backward(c):
        for a in range(3):
            for j in range(1, nx):
                cross(j, a, c).wait_recv()

        @pl.loop(0, half // 16)
        def _(r):
            sub = pl.ds(pl.multiple_of(r * 16, 16), 16)
            out = pl.ds(pl.multiple_of(mine + r * 16, 16), 16)
            back, gate, upper = [
                functools.reduce(
                    lambda u, v: u + v,
                    [xrec[j, a, c, sub, :].astype(f32) for j in range(1, nx)],
                    part[a, c, core, sub, :],
                )
                for a in range(3)
            ]
            logit = logbuf[out, 0:1]
            sig = jax.nn.sigmoid(gate)
            act = gate * sig
            slope = sig * (1.0 + gate * (1.0 - sig))
            hid_v = act * upper
            o_w[out, cols(c)] = (hid_v * logit).astype(bf16)
            d_hidden = logit * back
            o_dg[out, cols(c)] = (d_hidden * upper * slope).astype(bf16)
            o_du[out, cols(c)] = (d_hidden * act).astype(bf16)
            terms = hid_v * back
            add = terms[:, 0:128]
            for i in range(1, fc // 128):
                add = add + terms[:, i * 128 : (i + 1) * 128]
            rgacc[sub, :] = rgacc[sub, :] + add

        for a in range(3):
            act_copy(a, c).start()

    def kcols(k):
        return pl.ds(pl.multiple_of(k * kc, kc), kc)

    def back_dots(c, k):
        return nt_dot(o_dg[:, cols(c)], wg[kcols(k), cols(c)]) + nt_dot(
            o_du[:, cols(c)], wu[kcols(k), cols(c)]
        )

    def act_wait(c):
        for a in range(3):
            act_copy(a, c).wait_recv()

    @pl.loop(0, nc)
    def _(c):
        gate_backward(c)

        @pl.when(c > 0)
        def _():
            act_wait(c - 1)

            @pl.loop(0, nk)
            def _(k):
                acc[:, :, kcols(k)] = acc[:, :, kcols(k)] + back_dots(c - 1, k).reshape(
                    ns, cap, kc
                )

    rgbuf[core] = jnp.broadcast_to(jnp.sum(rgacc[...], axis=1, keepdims=True), (half, 128))
    rg_copy = remote(rgbuf.at[core], rgbuf.at[core], rg_s, rg_r, tensor=mate)
    rg_copy.start()
    act_wait(nc - 1)
    rg_copy.wait_recv()

    def ycopy(k):
        return remote(ysnd.at[k], yrec.at[k], y_s.at[k], y_r.at[k], seq=yp)

    def zcopy(j, k):
        return remote(
            zsnd.at[j, k],
            zrec.at[j, k],
            z_s.at[j, k],
            z_r.at[j, k],
            seq=2 * lax.rem(z + j, nz) + y,
        )

    def zstage(k):
        ycopy(k).wait_recv()
        for j in range(1, nz):
            zz = lax.rem(z + j, nz)
            zsnd[j, k] = (acc[2 * zz + y, :, kcols(k)] + yrec[k, zz].astype(f32)).astype(bf16)
            zcopy(j, k).start()
        acc[s, :, kcols(k)] = acc[s, :, kcols(k)] + yrec[k, z].astype(f32)

    @pl.loop(0, nk)
    def _(k):
        rg = jnp.concatenate([rgbuf[0], rgbuf[1]], axis=0)[:, 0:1]
        total = back_dots(nc - 1, k) + rg * router[:, kcols(k)]
        acc[:, :, kcols(k)] = acc[:, :, kcols(k)] + total.reshape(ns, cap, kc)
        for zz in range(nz):
            ysnd[k, zz] = acc[2 * zz + 1 - y, :, kcols(k)].astype(bf16)
        ycopy(k).start()

        @pl.when(k > 0)
        def _():
            zstage(k - 1)

    zstage(nk - 1)

    router_part = jnp.zeros((1, width), f32)
    count = jnp.zeros((1, 128), f32)
    rg_all = jnp.concatenate([rgbuf[0], rgbuf[1]], axis=0)
    for b in range(ns):
        block = o_norm[b * cap : (b + 1) * cap, :].astype(f32)
        router_part = router_part + jnp.sum(
            rg_all[b * cap : (b + 1) * cap, 0:1] * block, axis=0, keepdims=True
        )
        count = count + gath[b, 0:1, 2 * width : 2 * width + 128].astype(f32)
    scale = lax.rsqrt(count)
    o_cs[...] = scale
    gmsg[1:2, :] = router_part

    for j in range(1, nz):

        @pl.loop(0, nk)
        def _(k):
            zcopy(j, k).wait_recv()
            acc[s, :, kcols(k)] = acc[s, :, kcols(k)] + zrec[j, k].astype(f32)

    own = pl.ds(pl.multiple_of(s * cap, cap), cap)
    inverse = invbuf[own, 0:1]
    scaled = gath[s, :, pl.ds(0, width)].astype(f32) * inverse
    d_normed = acc[s]
    d_scaled = d_normed * gain[...]
    imsg[...] = jnp.broadcast_to(jnp.sum(d_scaled * scaled, axis=1, keepdims=True), (cap, 128))

    def inner_copy(j):
        return remote(imsg, irec.at[j], in_s.at[j], in_r.at[j], tensor=lax.rem(t + j, nt))

    def gain_copy(j):
        return remote(gmsg, grec.at[j], g_s.at[j], g_r.at[j], seq=lax.rem(s + j, ns))

    for j in range(1, nt):
        inner_copy(j).start()
    gmsg[0:1, :] = jnp.sum(d_normed * scaled, axis=0, keepdims=True)
    for j in range(1, ns):
        gain_copy(j).start()

    inner = imsg[...]
    for j in range(1, nt):
        inner_copy(j).wait_recv()
        inner = inner + irec[j]
    inner = inner[:, 0:1] / width_total
    d_picked = inverse * (d_scaled - scaled * inner) * live_col
    place = (tok_row[...] == lax.broadcasted_iota(jnp.int32, (tokens, cap), 0)).astype(f32)
    added = jnp.dot(place, d_picked, precision=lax.Precision.HIGHEST, preferred_element_type=f32)
    o_in[...] = (gout[...].astype(f32) + added).astype(bf16)

    total = gmsg[...]
    for j in range(1, ns):
        gain_copy(j).wait_recv()
        total = total + grec[j]
    o_gr[...] = total * scale[:, 0:1]

    agy(0).wait_send()
    for j in range(1, nz):
        agz(j).wait_send()
        agy(j).wait_send()
    for j in range(1, nt):
        small(0, j).wait_send()
        small(1, j).wait_send()
        inner_copy(j).wait_send()
    for j in range(1, ns):
        gain_copy(j).wait_send()
    rg_copy.wait_send()

    @pl.loop(0, nc)
    def _(c):
        for a in range(3):
            pair(a, c).wait_send()
            act_copy(a, c).wait_send()
            for j in range(1, nx):
                cross(j, a, c).wait_send()

    @pl.loop(0, nk)
    def _(k):
        ycopy(k).wait_send()
        for j in range(1, nz):
            zcopy(j, k).wait_send()


def body(
    hidden_in,
    grad_out,
    slot_tokens,
    live_counts,
    norm_gain,
    router_weight,
    gate_weight,
    up_weight,
    down_weight,
):
    ns, nt = lax.axis_size("seq"), lax.axis_size("tensor")
    cap = slot_tokens.shape[0]
    tokens, width = hidden_in.shape
    hidden = gate_weight.shape[1]
    rows, nz, nx = ns * cap, ns // 2, nt // 2
    half = rows // 2
    nc = pick_chunks(hidden, (6, 4, 3, 2))
    nk = pick_chunks(width, (4, 2))
    fc, kc = hidden // nc, width // nk
    vmem = pl.BlockSpec(memory_space=pltpu.VMEM)
    hbm = pl.BlockSpec(memory_space=pl.ANY)
    dma = pltpu.SemaphoreType.DMA
    grad_in, small, weighted, d_gate, d_up, normed, upstream, scale = pl.pallas_call(
        functools.partial(kernel, ns, nt, nc, nk),
        out_shape=[
            jax.ShapeDtypeStruct((tokens, width), bf16),
            jax.ShapeDtypeStruct((2, width), f32),
            jax.ShapeDtypeStruct((rows, hidden), bf16),
            jax.ShapeDtypeStruct((rows, hidden), bf16),
            jax.ShapeDtypeStruct((rows, hidden), bf16),
            jax.ShapeDtypeStruct((rows, width), bf16),
            jax.ShapeDtypeStruct((rows, width), bf16),
            jax.ShapeDtypeStruct((1, 128), f32),
        ],
        in_specs=[vmem] * 7 + [hbm] * 3,
        out_specs=[vmem] * 8,
        scratch_shapes=[
            pltpu.VMEM((width, hidden), bf16),
            pltpu.VMEM((width, hidden), bf16),
            pltpu.VMEM((hidden, width), bf16),
            pltpu.VMEM((ns, cap, 2 * width + 128), bf16),
            pltpu.VMEM((rows, 128), f32),
            pltpu.VMEM((rows, 128), f32),
            pltpu.VMEM((rows, 128), f32),
            pltpu.VMEM((2, half, 128), f32),
            pltpu.VMEM((half, 128), f32),
            pltpu.VMEM((2, 8, rows), f32),
            pltpu.VMEM((2, nt, 8, rows), f32),
            pltpu.VMEM((cap, 128), f32),
            pltpu.VMEM((nt, cap, 128), f32),
            pltpu.VMEM((3, nc, 2, half, fc), f32),
            pltpu.VMEM((3, nc, half, fc), f32),
            pltpu.VMEM((3, nc, half, fc), bf16),
            pltpu.VMEM((nx, 3, nc, half, fc), bf16),
            pltpu.VMEM((ns, cap, width), f32),
            pltpu.VMEM((nk, nz, cap, kc), bf16),
            pltpu.VMEM((nk, nz, cap, kc), bf16),
            pltpu.VMEM((nz, nk, cap, kc), bf16),
            pltpu.VMEM((nz, nk, cap, kc), bf16),
            pltpu.VMEM((2, width), f32),
            pltpu.VMEM((ns, 2, width), f32),
            dma((3,)),
            dma((nz,)),
            dma((nz,)),
            dma((nz,)),
            dma((nz,)),
            dma((2, nt)),
            dma((2, nt)),
            dma((nt,)),
            dma((nt,)),
            dma((3, nc)),
            dma((3, nc)),
            dma((nx, 3, nc)),
            dma((nx, 3, nc)),
            dma((3, nc)),
            dma((3, nc)),
            dma,
            dma,
            dma((nk,)),
            dma((nk,)),
            dma((nz, nk)),
            dma((nz, nk)),
            dma((ns,)),
            dma((ns,)),
        ],
        compiler_params=pltpu.CompilerParams(
            collective_id=0, has_side_effects=True, vmem_limit_bytes=67_043_328
        ),
    )(
        hidden_in,
        grad_out,
        slot_tokens.reshape(cap, 1),
        slot_tokens.reshape(1, cap),
        live_counts.reshape(1, 1),
        norm_gain.reshape(1, width),
        router_weight.reshape(1, width),
        gate_weight,
        up_weight,
        down_weight,
    )
    grad_gate, grad_up, grad_down = outer_products(
        normed, d_gate, d_up, weighted, upstream, scale
    )
    return (grad_in, grad_gate, grad_up, grad_down, small[0], small[1])


def solution(mesh):
    in_specs = (
        P("seq", "tensor"),
        P("seq", "tensor"),
        P("seq"),
        P("seq"),
        P("tensor"),
        P("tensor"),
        P("tensor", "seq"),
        P("tensor", "seq"),
        P("seq", "tensor"),
    )
    out_specs = (
        P("seq", "tensor"),
        P("tensor", "seq"),
        P("tensor", "seq"),
        P("seq", "tensor"),
        P("tensor"),
        P("tensor"),
    )
    return jax.shard_map(body, mesh=mesh, in_specs=in_specs, out_specs=out_specs, check_vma=False)
```
